128 devices in a mesh: sx: 16 (over x, z_hi, core), sy: 8 (over z_lo, y).
Axes of the slice: x: 4, y: 4, z: 4 (z_hi: 2, z_lo: 2; z = z_hi * 2 + z_lo), core: 2. Of those that a mesh axis runs over, the one named last changes fastest.
Arguments:
- tokens: bfloat16 [65536, 1024], P(('sx', 'sy')), may hold values from -6 to 6
- norm_gain: float32 [1024], replicated, may hold values from 0.1 to 1.9
- w_qk: bfloat16 [1024, 1024], replicated, may hold values from -1.75 to 1.75
- w_value: bfloat16 [1024, 1024], replicated, may hold values from -0.1875 to 0.1875
- w_out: bfloat16 [1024, 1024], replicated, may hold values from -0.1875 to 0.1875
- send_order: int32 [8, 65536], P(None, ('sx', 'sy')), may hold values from 0 to 511, as said below
- place: int32 [8, 65536], P(None, ('sx', 'sy')), may hold values from 0 to 511, as said below
Outputs:
- attended: bfloat16 [65536, 1024], P(('sx', 'sy'))
The draws below stay inside these ranges and needn't reach their ends.
Inputs may be any that keep to these rules, and one draw needn't show every extreme that they name: `send_order`: for every head and every device, the device's 512 entries form a permutation of 0 to 511. `place`: for every head and every device, the device's 512 entries form a permutation of 0 to 511.
All inputs are finite; a program needn't handle non-finite values.
Results may differ from the reference program's by a relative error of at most 0.012.
The reference program's roundings to bfloat16 on the way count: a program that leaves them out, or rounds other values in their place, can miss the bound.
Values may be sent and summed in bfloat16 or wider, within the bound.
A program may use at most 64 MiB of HBM per device.

```python
import jax
import jax.numpy as jnp
from jax import lax

D = 1024
HEADS = 8
HEAD_DIM = 128
SPAN = 128
TOK_DEV = 512
TOKENS = 65536
N_SX = 16
N_SY = 8


def block_permutations(key):
    keys = jax.random.split(key, HEADS * N_SX * N_SY)
    perms = jax.vmap(lambda single: jax.random.permutation(single, TOK_DEV))(keys)
    return perms.reshape(HEADS, TOKENS).astype(jnp.int32)


def draw_send_order(key, part):
    return block_permutations(jax.random.fold_in(key, 11))


def draw_place(key, part):
    return block_permutations(jax.random.fold_in(key, 23))


def draw_w_qk(key, part):
    sigma = (D // 64) ** (-0.5)
    base = jax.random.normal(jax.random.fold_in(key, 53), (D, D), dtype=jnp.float32) * sigma
    base = jnp.clip(base, -6.0 * sigma, 6.0 * sigma)
    return base.astype(jnp.bfloat16)


def draw_tokens(key, part):
    noise = jax.random.normal(jax.random.fold_in(key, 61), (TOKENS, D), dtype=jnp.float32)
    noise = jnp.clip(noise, -6.0, 6.0)
    return noise.astype(jnp.bfloat16)


def gaussian(own_key, extent, width, reach, kind=jnp.bfloat16):
    drawn = width * jax.random.normal(own_key, extent, jnp.float32)
    return jnp.clip(drawn, min=-reach, max=reach).astype(kind)


def setup_inputs(seed: int = 0) -> dict:
    streams_of = jax.random.split(jax.random.key(seed), 8)
    return {
        "tokens": draw_tokens(jax.random.fold_in(streams_of[7], 71), 0),
        "norm_gain": jnp.clip(1.0 + 0.18 * jax.random.normal(streams_of[1], (D,), jnp.float32), 0.1, 1.9),
        "w_qk": draw_w_qk(jax.random.fold_in(streams_of[7], 71), 0),
        "w_value": gaussian(streams_of[3], (D, D), D ** -0.5, 0.1875),
        "w_out": gaussian(streams_of[4], (D, D), D ** -0.5, 0.1875),
        "send_order": draw_send_order(jax.random.fold_in(streams_of[7], 71), 0),
        "place": draw_place(jax.random.fold_in(streams_of[7], 71), 0),
    }


def bucket_order(send_order, place):
    ndev = N_SX * N_SY
    peer = TOK_DEV // ndev
    sent = send_order.reshape(HEADS, ndev, ndev, peer)
    source = sent + (jnp.arange(ndev, dtype=jnp.int32) * TOK_DEV)[None, :, None, None]
    source = source.transpose(0, 2, 1, 3).reshape(HEADS, TOKENS)
    target = place.reshape(HEADS, ndev, TOK_DEV) + (jnp.arange(ndev, dtype=jnp.int32) * TOK_DEV)[None, :, None]
    target = target.reshape(HEADS, TOKENS)
    heads_idx = jnp.arange(HEADS, dtype=jnp.int32)[:, None]
    return jnp.zeros((HEADS, TOKENS), jnp.int32).at[heads_idx, target].set(source)

def attend_spans(current, previous):
    window = jnp.concatenate([previous, current], axis=1)
    query = current[..., :HEAD_DIM].astype(jnp.float32)
    keys = window[..., :HEAD_DIM].astype(jnp.float32)
    key_stat = lax.optimization_barrier(jnp.sum(keys * keys, -1, keepdims=True)) + 1e-06
    unit = (keys * lax.rsqrt(key_stat)).astype(jnp.bfloat16)
    scores = jnp.einsum('cqd,ckd->cqk', query, unit.astype(jnp.float32)) * HEAD_DIM ** (-0.5)
    rows = jnp.arange(SPAN)[:, None]
    cols = jnp.arange(2 * SPAN)[None, :]
    scores = jnp.where(cols == rows + SPAN, -100000.0, scores)
    weights = jax.nn.softmax(scores, axis=-1).astype(jnp.bfloat16)
    vals = window[..., HEAD_DIM:].astype(jnp.float32)
    return jnp.einsum('cqk,ckd->cqd', weights.astype(jnp.float32), vals).astype(jnp.bfloat16)

def reference(tokens, norm_gain, w_qk, w_value, w_out, send_order, place):
    floats = tokens.astype(jnp.float32)
    row_stat = lax.optimization_barrier(jnp.mean(floats * floats, -1, keepdims=True)) + 1e-06
    scale = lax.rsqrt(row_stat)
    normed = (floats * scale * norm_gain.astype(jnp.float32)).astype(jnp.bfloat16)
    shared = jnp.dot(normed, w_qk, preferred_element_type=jnp.float32).astype(jnp.bfloat16)
    values = jnp.dot(normed, w_value, preferred_element_type=jnp.float32).astype(jnp.bfloat16)
    stacked = jnp.concatenate([shared.reshape(TOKENS, HEADS, HEAD_DIM), values.reshape(TOKENS, HEADS, HEAD_DIM)], -1)
    stacked = stacked.transpose(1, 0, 2)
    order = bucket_order(send_order, place)

    def one_head(pair):
        rows, index = pair
        ordered = rows[index].reshape(TOKENS // SPAN, SPAN, 2 * HEAD_DIM)
        previous = jnp.roll(ordered, 1, axis=0)
        result = attend_spans(ordered, previous).reshape(TOKENS, HEAD_DIM)
        return jnp.zeros((TOKENS, HEAD_DIM), jnp.bfloat16).at[index].set(result)
    heads_out = lax.map(one_head, (stacked, order))
    merged = heads_out.transpose(1, 0, 2).reshape(TOKENS, D)
    return jnp.dot(merged, w_out, preferred_element_type=jnp.float32).astype(jnp.bfloat16)
```

```python
import jax
import jax.numpy as jnp
from jax import lax
from jax.experimental import pallas as pl
from jax.experimental.pallas import tpu as pltpu
from jax.sharding import PartitionSpec as P

MESH = pl.DeviceIdType.MESH
F32, BF16, I32 = jnp.float32, jnp.bfloat16, jnp.int32
D, HEADS, HD, SPAN, TOK = 1024, 8, 128, 128, 512
NSX, NSY = 16, 8
NDEV = NSX * NSY
NPOS = 8 * TOK
SCALE = HD ** (-0.5)


def place_of(dxc, dyz):
    sx, sy = lax.axis_index("sx"), lax.axis_index("sy")
    x = lax.rem(sx // 4 + lax.rem(dxc, 4), 4)
    core = lax.rem(lax.rem(sx, 2) + dxc // 4, 2)
    y = lax.rem(lax.rem(sy, 4) + lax.rem(dyz, 4), 4)
    z = lax.rem(lax.rem(sx // 2, 2) * 2 + sy // 4 + dyz // 4, 4)
    return x * 4 + (z // 2) * 2 + core, lax.rem(z, 2) * 4 + y


def signal(sem, target):
    pl.semaphore_signal(sem, inc=1, device_id=target, device_id_type=MESH)


def swapped(rows):
    lane = lax.broadcasted_iota(I32, rows.shape, 1)
    width = rows.shape[1]
    return jnp.where((lane // 4) % 2 == 0, pltpu.roll(rows, width - 4, 1), pltpu.roll(rows, 4, 1))


def spread(columns, out_ref):
    for j in range(8):
        out_ref[j] = jnp.broadcast_to(columns[:, j : j + 1], (TOK, 128))


def hot_rows(column):
    lane = lax.broadcasted_iota(I32, (TOK, 128), 1)
    return jnp.concatenate(
        [jnp.where(column == lane + 128 * c, 1.0, 0.0).astype(BF16) for c in range(TOK // 128)], axis=1
    )


def hot_columns(row):
    token = lax.broadcasted_iota(I32, (TOK, TOK), 0)
    return jnp.where(token == row, 1.0, 0.0).astype(BF16)


def dot(a, b):
    return jnp.dot(a, b, preferred_element_type=F32)


def halves(first, second):
    low = lax.broadcasted_iota(I32, first.shape, 1) < 4
    return jnp.where(low, first, second)


def kernel(
    tokens_hbm, gain_ref, wqk_hbm, wv_hbm, wo_hbm, send_ref, place_ref, out_ref,
    tokens, wqk, wv, wo, normed, outgoing, arrived, leaving, returned, placein, placerow,
    sendcol, placecol, sendrow, mergehot, orderhot, leavehot, ordered, unit, sorted_out, merged,
    load_sem, met_sem, place_s, place_r, out_s, out_r, halo_s, halo_r, back_s, back_r,
):
    sx, sy = lax.axis_index("sx"), lax.axis_index("sy")
    me = sx * NSY + sy

    barrier = pltpu.get_barrier_semaphore()
    for dxc in range(1, 8):
        signal(barrier, place_of(dxc, 0))
    for dyz in range(1, 16):
        signal(barrier, place_of(0, dyz))

    loads = [
        pltpu.make_async_copy(src, dst, load_sem.at[n])
        for n, (src, dst) in enumerate([(tokens_hbm, tokens), (wqk_hbm, wqk), (wv_hbm, wv), (wo_hbm, wo)])
    ]
    for load in loads:
        load.start()

    send = send_ref[...]
    send = jnp.where(lax.rem(sy, 2) == 1, swapped(send), send)
    sendrow[...] = send
    spread(send.T, sendcol)

    loads[0].wait()

    def norm(i, _):
        at = pl.ds(pl.multiple_of(i * 64, 64), 64)
        rows = tokens[at, :].astype(F32)
        stat = jnp.mean(rows * rows, -1, keepdims=True) + 1e-06
        normed[at, :] = (rows * lax.rsqrt(stat) * gain_ref[...]).astype(BF16)
        return 0

    lax.fori_loop(0, TOK // 64, norm, 0)
    loads[1].wait()
    loads[2].wait()

    def project(h, _):
        at = pl.ds(pl.multiple_of(h * HD, HD), HD)
        weight = jnp.concatenate([wqk[:, at], wv[:, at]], axis=1)
        both = dot(normed[...], weight).astype(BF16)
        outgoing[h] = dot(hot_rows(sendcol[h]), both).astype(BF16)
        return 0

    lax.fori_loop(0, HEADS, project, 0)

    pl.semaphore_wait(barrier, 7 + 15)
    for dxc in range(1, 8):
        signal(met_sem, place_of(dxc, 0))

    def send_place(k, _):
        pltpu.make_async_remote_copy(
            place_ref, placein.at[sy], place_s, place_r, device_id=(sx, lax.rem(sy + k, NSY)), device_id_type=MESH
        ).start()
        return 0

    lax.fori_loop(1, NSY, send_place, 0)
    placein[sy] = place_ref[...]

    def send_rows(tx, ty):
        pltpu.make_async_remote_copy(
            outgoing.at[ty, pl.ds(pl.multiple_of(tx * 32, 32), 32)],
            arrived.at[me],
            out_s,
            out_r,
            device_id=(tx, ty),
            device_id_type=MESH,
        ).start()

    def send_near(i, _):
        send_rows(*place_of(i, 0))
        return 0

    def send_plane(i, _):
        send_rows(*place_of(0, i))
        return 0

    def send_far(i, _):
        send_rows(*place_of(1 + lax.rem(i, 7), 1 + lax.rem(i, 15)))
        return 0

    lax.fori_loop(1, 8, send_near, 0)
    lax.fori_loop(1, 16, send_plane, 0)
    pl.semaphore_wait(met_sem, 7)
    lax.fori_loop(0, 105, send_far, 0)
    arrived[me] = outgoing[sy, pl.ds(pl.multiple_of(sx * 32, 32), 32), :]

    def table(h, _):
        mergehot[h] = hot_columns(sendrow[pl.ds(h, 1), :])
        return 0

    lax.fori_loop(0, HEADS, table, 0)
    whole_place = pltpu.make_async_remote_copy(
        placein.at[pl.ds(0, NSY - 1)], placein.at[pl.ds(0, NSY - 1)], place_s, place_r, device_id=(sx, sy),
        device_id_type=MESH,
    )
    whole_place.wait_send()
    whole_place.wait_recv()
    for j in range(8):
        placerow[j : j + 1, :] = placein[j, pl.ds(sy, 1), :]
    block = lax.broadcasted_iota(I32, (8, TOK), 0)
    placerow[...] = jnp.where(block % 2 == 1, swapped(placerow[...]), placerow[...])
    spread(placerow[...].T, placecol)

    def place_table(j, _):
        orderhot[j] = hot_columns(placerow[pl.ds(j, 1), :])
        leavehot[j] = hot_rows(placecol[j])
        return 0

    lax.fori_loop(0, 8, place_table, 0)

    whole_out = pltpu.make_async_remote_copy(
        arrived.at[pl.ds(0, NDEV - 1)], arrived.at[pl.ds(0, NDEV - 1)], out_s, out_r, device_id=(sx, sy),
        device_id_type=MESH,
    )
    whole_out.wait_send()
    whole_out.wait_recv()

    def order(n, _):
        half = 1 - n
        rows = arrived[:, pl.ds(pl.multiple_of(half * 16, 16), 16), :].astype(F32)
        for sub in (1, 0):
            group = rows[:, sub * 8 : sub * 8 + 8, :].reshape(NDEV // 2, 2, 8, 2 * HD)
            even, odd = group[:, 0], group[:, 1]
            for b, pair in ((1, (odd, even)), (0, (even, odd))):
                j = half * 4 + sub * 2 + b
                mixed = halves(*pair).reshape(TOK, 2 * HD).astype(BF16)
                at = pl.ds(pl.multiple_of(SPAN + j * TOK, SPAN), TOK)
                ordered[at, :] = dot(orderhot[j], mixed).astype(BF16)
        return 0

    lax.fori_loop(0, 2, order, 0)
    halo = pltpu.make_async_remote_copy(
        ordered.at[pl.ds(NPOS, SPAN)], ordered.at[pl.ds(0, SPAN)], halo_s, halo_r,
        device_id=(lax.rem(sx + 1, NSX), sy), device_id_type=MESH,
    )
    halo.start()

    def units(i, _):
        at = pl.ds(pl.multiple_of(i * SPAN, SPAN), SPAN)
        keys = ordered[at, :HD].astype(F32)
        stat = jnp.sum(keys * keys, -1, keepdims=True) + 1e-06
        unit[at, :] = (keys * lax.rsqrt(stat)).astype(BF16)
        return 0

    def attend(c, _):
        at = pl.ds(pl.multiple_of(c * SPAN, SPAN), 2 * SPAN)
        query = ordered[pl.ds(pl.multiple_of(c * SPAN + SPAN, SPAN), SPAN), :HD]
        scores = lax.dot_general(query, unit[at, :], (((1,), (1,)), ((), ())), preferred_element_type=F32) * SCALE
        rows = lax.broadcasted_iota(I32, (SPAN, 2 * SPAN), 0)
        cols = lax.broadcasted_iota(I32, (SPAN, 2 * SPAN), 1)
        scores = jnp.where(cols == rows + SPAN, -100000.0, scores)
        peak = jnp.max(scores, -1, keepdims=True)
        grown = jnp.exp(scores - peak)
        weights = (grown / jnp.sum(grown, -1, keepdims=True)).astype(BF16)
        sorted_out[pl.ds(pl.multiple_of(c * SPAN, SPAN), SPAN), :] = dot(weights, ordered[at, HD:]).astype(BF16)
        return 0

    lax.fori_loop(1, 33, units, 0)
    lax.fori_loop(1, 32, attend, 0)
    halo.wait_send()
    halo.wait_recv()
    units(0, 0)
    attend(0, 0)

    def leave(half, _):
        tiles = []
        for sub in range(2):
            parts = []
            for b in range(2):
                j = half * 4 + sub * 2 + b
                rows = sorted_out[pl.ds(pl.multiple_of(j * TOK, TOK), TOK), :]
                parts.append(dot(leavehot[j], rows).reshape(NDEV // 2, 8, HD))
            pair = jnp.stack([halves(parts[0], parts[1]), halves(parts[1], parts[0])], axis=1)
            tiles.append(pair.reshape(NDEV, 8, HD))
        leaving[:, pl.ds(pl.multiple_of(half * 16, 16), 16), :] = jnp.concatenate(tiles, axis=1).astype(BF16)
        return 0

    lax.fori_loop(0, 2, leave, 0)

    def send_back(tx, ty):
        pltpu.make_async_remote_copy(
            leaving.at[tx * NSY + ty],
            returned.at[sy, pl.ds(pl.multiple_of(sx * 32, 32), 32)],
            back_s,
            back_r,
            device_id=(tx, ty),
            device_id_type=MESH,
        ).start()

    def back_far(i, _):
        send_back(*place_of(1 + lax.rem(i, 7), 1 + lax.rem(i, 15)))
        return 0

    def back_near(i, _):
        send_back(*place_of(i, 0))
        return 0

    def back_plane(i, _):
        send_back(*place_of(0, i))
        return 0

    lax.fori_loop(0, 105, back_far, 0)
    lax.fori_loop(1, 16, back_plane, 0)
    lax.fori_loop(1, 8, back_near, 0)
    returned[sy, pl.ds(pl.multiple_of(sx * 32, 32), 32), :] = leaving[me]
    loads[3].wait()
    whole_back = pltpu.make_async_remote_copy(
        leaving.at[pl.ds(0, NDEV - 1)], leaving.at[pl.ds(0, NDEV - 1)], back_s, back_r, device_id=(sx, sy),
        device_id_type=MESH,
    )
    whole_back.wait_send()
    whole_back.wait_recv()

    def merge(h, _):
        merged[:, pl.ds(pl.multiple_of(h * HD, HD), HD)] = dot(mergehot[h], returned[h]).astype(BF16)
        return 0

    lax.fori_loop(0, HEADS, merge, 0)

    def project_out(n, _):
        at = pl.ds(pl.multiple_of(n * 256, 256), 256)
        out_ref[:, at] = dot(merged[...], wo[:, at]).astype(BF16)
        return 0

    lax.fori_loop(0, D // 256, project_out, 0)


def per_device(tokens, norm_gain, w_qk, w_value, w_out, send_order, place):
    vmem = pl.BlockSpec(memory_space=pltpu.VMEM)
    hbm = pl.BlockSpec(memory_space=pl.ANY)
    dma = pltpu.SemaphoreType.DMA
    return pl.pallas_call(
        kernel,
        out_shape=jax.ShapeDtypeStruct((TOK, D), BF16),
        in_specs=[hbm, vmem, hbm, hbm, hbm, vmem, vmem],
        out_specs=vmem,
        scratch_shapes=[
            pltpu.VMEM((TOK, D), BF16),
            pltpu.VMEM((D, D), BF16),
            pltpu.VMEM((D, D), BF16),
            pltpu.VMEM((D, D), BF16),
            pltpu.VMEM((TOK, D), BF16),
            pltpu.VMEM((HEADS, TOK, 2 * HD), BF16),
            pltpu.VMEM((NDEV, 32, 2 * HD), BF16),
            pltpu.VMEM((NDEV, 32, HD), BF16),
            pltpu.VMEM((HEADS, TOK, HD), BF16),
            pltpu.VMEM((NSY, HEADS, TOK), I32),
            pltpu.VMEM((8, TOK), I32),
            pltpu.VMEM((8, TOK, 128), I32),
            pltpu.VMEM((8, TOK, 128), I32),
            pltpu.VMEM((8, TOK), I32),
            pltpu.VMEM((HEADS, TOK, TOK), BF16),
            pltpu.VMEM((8, TOK, TOK), BF16),
            pltpu.VMEM((8, TOK, TOK), BF16),
            pltpu.VMEM((NPOS + SPAN, 2 * HD), BF16),
            pltpu.VMEM((NPOS + SPAN, HD), BF16),
            pltpu.VMEM((NPOS, HD), BF16),
            pltpu.VMEM((TOK, D), BF16),
            dma((4,)),
            pltpu.SemaphoreType.REGULAR,
            dma, dma, dma, dma, dma, dma, dma, dma,
        ],
        compiler_params=pltpu.CompilerParams(
            collective_id=0, has_side_effects=True, vmem_limit_bytes=60 * 2**20
        ),
    )(tokens, norm_gain.reshape(1, D), w_qk, w_value, w_out, send_order, place)


def solution(mesh):
    return jax.shard_map(
        per_device,
        mesh=mesh,
        in_specs=(P(("sx", "sy"), None), P(), P(), P(), P(), P(None, ("sx", "sy")), P(None, ("sx", "sy"))),
        out_specs=P(("sx", "sy"), None),
        check_vma=False,
    )
```

```python
import random

import jax
import jax.numpy as jnp
from jax import lax
from jax.experimental import pallas as pl
from jax.experimental.pallas import tpu as pltpu
from jax.sharding import PartitionSpec as P

MESH = pl.DeviceIdType.MESH
F32, BF16, I32 = jnp.float32, jnp.bfloat16, jnp.int32
D, HEADS, HD, SPAN, TOK = 1024, 8, 128, 128, 512
NSX, NSY = 16, 8
NDEV = NSX * NSY
NPOS = 8 * TOK
GROUP = 4
VMEM_LIMIT = 44 * 2**20
SCALE = HD ** (-0.5)
LOG2E = 1.4426950408889634
scope = jax.named_scope


def offsets():
    every = [
        (dx, hi, core, lo, dy)
        for dx in range(4) for hi in range(2) for core in range(2) for lo in range(2) for dy in range(4)
    ][1:]
    random.Random(1).shuffle(every)
    every.sort(key=lambda o: -(min(o[0], 4 - o[0]) + min(o[4], 4 - o[4]) + (1 if o[3] else 2 * o[1])))
    return [o for o in every if not (o[3] or o[4])], [o for o in every if o[3] or o[4]]


def reach(sx, sy):
    xs = [lax.rem(sx // 4 + d, 4) * 4 for d in range(4)]
    hi, core, lo = lax.rem(sx // 2, 2), lax.rem(sx, 2), sy // 4
    pairs = [[(1 - hi if a else hi) * 2 + (1 - core if b else core) for b in range(2)] for a in range(2)]
    txs = [[[xs[d] + pairs[a][b] for b in range(2)] for a in range(2)] for d in range(4)]
    tys = [[(1 - lo if a else lo) * 4 + lax.rem(lax.rem(sy, 4) + d, 4) for d in range(4)] for a in range(2)]
    return lambda o: (txs[o[0]][o[1]][o[2]], tys[o[3]][o[4]])


def signal(sem, target):
    pl.semaphore_signal(sem, inc=1, device_id=target, device_id_type=MESH)


def swapped(rows):
    lane = lax.broadcasted_iota(I32, rows.shape, 1)
    width = rows.shape[1]
    return jnp.where((lane // 4) % 2 == 0, pltpu.roll(rows, width - 4, 1), pltpu.roll(rows, 4, 1))


def spread(columns, out_ref):
    for j in range(8):
        out_ref[j] = jnp.broadcast_to(columns[:, j : j + 1], (TOK, 128))


def hot_rows(column):
    lane = lax.broadcasted_iota(I32, (TOK, 128), 1)
    return jnp.concatenate(
        [jnp.where(column == lane + 128 * c, 1.0, 0.0).astype(BF16) for c in range(TOK // 128)], axis=1
    )


def hot_columns(row):
    token = lax.broadcasted_iota(I32, (TOK, row.shape[1]), 0)
    return jnp.where(token == row, 1.0, 0.0).astype(BF16)


def dot(a, b):
    return jnp.dot(a, b, preferred_element_type=F32)


def halves(first, second):
    low = lax.broadcasted_iota(I32, first.shape, 1) < 4
    return jnp.where(low, first, second)


def kernel(
    tokens_hbm, gain_hbm, wqk_hbm, wv_hbm, send_hbm, place_hbm, merged,
    tokens, gain, wqk, wv, send_ref, place_ref, normed, outgoing, arrived, leaving, returned, placeout, placein, placerow,
    sendcol, placecol, sendrow, mergehot, orderhot, leavehot, ordered, unit, sorted_out,
    load_sem, met_sem, place_s, place_r, out_s, out_r, halo_s, halo_r, back_s, back_r,
):
    sx, sy = lax.axis_index("sx"), lax.axis_index("sy")
    me = sx * NSY + sy
    at_offset = reach(sx, sy)
    line, rest = offsets()

    with scope("signal"):
        barrier = pltpu.get_barrier_semaphore()
        for k in range(1, NSX):
            signal(barrier, (lax.rem(sx + k, NSX), sy))
        for k in range(1, NSY):
            signal(barrier, (sx, lax.rem(sy + k, NSY)))
        loads = [
            pltpu.make_async_copy(src, dst, load_sem.at[n])
            for n, (src, dst) in enumerate([
                (send_hbm, send_ref), (place_hbm, place_ref), (gain_hbm, gain),
                (tokens_hbm, tokens), (wqk_hbm, wqk), (wv_hbm, wv),
            ])
        ]
        for load in loads:
            load.start()

    with scope("index"):
        loads[0].wait()
        loads[1].wait()
        send = send_ref[...]
        send = jnp.where(lax.rem(sy, 2) == 1, swapped(send), send)
        sendrow[...] = send
        spread(send.T, sendcol)
        for h in range(HEADS):
            placeout[h] = place_ref[h : h + 1, :]

    with scope("norm"):
        loads[2].wait()
        loads[3].wait()

        def norm(i, _):
            at = pl.ds(pl.multiple_of(i * 128, 128), 128)
            rows = tokens[at, :].astype(F32)
            stat = jnp.mean(rows * rows, -1, keepdims=True) + 1e-06
            normed[at, :] = (rows * lax.rsqrt(stat) * gain[...]).astype(BF16)
            return 0

        lax.fori_loop(0, TOK // 128, norm, 0)

    with scope("waitw"):
        loads[4].wait()
        loads[5].wait()

    def project(lo, dy):
        h = at_offset((0, 0, 0, lo, dy))[1]
        at = pl.ds(pl.multiple_of(h * HD, HD), HD)
        weight = jnp.concatenate([wqk[:, at], wv[:, at]], axis=1)
        both = dot(normed[...], weight).astype(BF16)
        rows = dot(hot_rows(sendcol[h]), both)
        outgoing[h] = rows.reshape(NSX, 4, 8, 2 * HD).astype(BF16)

    def send_rows(first, count, sem, target):
        tx, ty = target
        pltpu.make_async_remote_copy(
            outgoing.at[ty, tx, pl.ds(first, count)],
            arrived.at[me, pl.ds(first, count)],
            out_s.at[sem],
            out_r.at[sem],
            device_id=target,
            device_id_type=MESH,
        ).start()

    with scope("project0"):
        project(0, 0)

    with scope("barrier1"):
        pl.semaphore_wait(barrier, NSX - 1 + NSY - 1)
        for k in range(1, NSY):
            signal(met_sem, (sx, lax.rem(sy + k, NSY)))

    with scope("send_near"):
        for o in line:
            send_rows(1, 3, 0, at_offset(o))
        for k in range(1, NSY):
            ty = lax.rem(sy + k, NSY)
            pltpu.make_async_remote_copy(
                placeout.at[ty], placein.at[sy], place_s, place_r, device_id=(sx, ty), device_id_type=MESH
            ).start()

    with scope("project1"):
        for dy in (1, 2, 3):
            project(0, dy)

    with scope("barrier2"):
        pl.semaphore_wait(met_sem, NSY - 1)

    with scope("send_mid"):
        for o in [o for o in rest if not o[3]]:
            send_rows(1, 3, 0, at_offset(o))

    with scope("project2"):
        for dy in range(4):
            project(1, dy)

    with scope("send_far"):
        for o in [o for o in rest if o[3]]:
            send_rows(1, 3, 0, at_offset(o))
        for o in rest + line:
            send_rows(0, 1, 1, at_offset(o))
        arrived[me] = outgoing[sy, sx]

    with scope("tables"):
        def table(h, _):
            mergehot[h] = hot_columns(sendrow[pl.ds(h, 1), :])
            return 0

        lax.fori_loop(0, HEADS, table, 0)
        whole_place = pltpu.make_async_remote_copy(
            placein.at[pl.ds(0, NSY - 1)], placein.at[pl.ds(0, NSY - 1)], place_s, place_r, device_id=(sx, sy),
            device_id_type=MESH,
        )
        whole_place.wait_send()
        whole_place.wait_recv()
        placein[sy] = placeout[sy]
        for j in range(8):
            placerow[j : j + 1, :] = placein[j]
        block = lax.broadcasted_iota(I32, (8, TOK), 0)
        placerow[...] = jnp.where(block % 2 == 1, swapped(placerow[...]), placerow[...])
        spread(placerow[...].T, placecol)

        def place_table(j, _):
            orderhot[j] = hot_columns(placerow[pl.ds(j, 1), :])
            leavehot[j] = hot_rows(placecol[j])
            return 0

        lax.fori_loop(0, 8, place_table, 0)

    def wait_all(ref, send_sem, recv_sem):
        whole = pltpu.make_async_remote_copy(
            ref, ref, send_sem, recv_sem, device_id=(sx, sy), device_id_type=MESH
        )
        whole.wait_send()
        whole.wait_recv()

    def units(keys, at):
        stat = jnp.sum(keys * keys, -1, keepdims=True) + 1e-06
        unit[at, :] = (keys * lax.rsqrt(stat)).astype(BF16)

    def order(q):
        group = arrived[:, q].astype(F32).reshape(NDEV // 2, 2, 8, 2 * HD)
        even, odd = group[:, 0], group[:, 1]
        for b, pair in ((1, (odd, even)), (0, (even, odd))):
            j = 2 * q + b
            mixed = halves(*pair).reshape(TOK, 2 * HD).astype(BF16)
            at = pl.ds(SPAN + j * TOK, TOK)
            rows = dot(orderhot[j], mixed)
            ordered[at, :] = rows.astype(BF16)
            units(rows[:, :HD], at)

    def attend(g, _):
        diagonal = lax.broadcasted_iota(I32, (SPAN, SPAN), 0) == lax.broadcasted_iota(I32, (SPAN, SPAN), 1)
        for u in range(GROUP):
            c = g * GROUP + u
            at = pl.ds(pl.multiple_of(c * SPAN, SPAN), 2 * SPAN)
            query = ordered[pl.ds(pl.multiple_of(c * SPAN + SPAN, SPAN), SPAN), :HD]
            scores = lax.dot_general(query, unit[at, :], (((1,), (1,)), ((), ())), preferred_element_type=F32)
            before, own = scores[:, :SPAN], jnp.where(diagonal, -100000.0 / SCALE, scores[:, SPAN:])
            peak = jnp.max(jnp.maximum(before, own), -1, keepdims=True)
            before, own = jnp.exp2((before - peak) * (SCALE * LOG2E)), jnp.exp2((own - peak) * (SCALE * LOG2E))
            share = 1.0 / jnp.sum(before + own, -1, keepdims=True)
            weights = jnp.concatenate([before * share, own * share], axis=1).astype(BF16)
            sorted_out[pl.ds(pl.multiple_of(c * SPAN, SPAN), SPAN), :] = dot(weights, ordered[at, HD:]).astype(BF16)
        return 0

    def leave(q):
        parts = []
        for b in range(2):
            j = q * 2 + b
            rows = sorted_out[pl.ds(j * TOK, TOK), :]
            parts.append(dot(leavehot[j], rows).reshape(NDEV // 2, 8, HD))
        pair = jnp.stack([halves(parts[0], parts[1]), halves(parts[1], parts[0])], axis=1)
        leaving[:, q] = pair.reshape(NDEV, 8, HD).astype(BF16)

    def send_back(first, target, sem):
        tx, ty = target
        pltpu.make_async_remote_copy(
            leaving.at[tx * NSY + ty, pl.ds(first, 2)],
            returned.at[sy, sx, pl.ds(first, 2)],
            back_s.at[sem],
            back_r.at[sem],
            device_id=target,
            device_id_type=MESH,
        ).start()

    def send_all_back(first, sem):
        for o in rest + line:
            send_back(first, at_offset(o), sem)

    with scope("wait_out0"):
        wait_all(arrived.at[pl.ds(0, NDEV - 1), pl.ds(0, 3)], out_s.at[0], out_r.at[0])

    with scope("order0"):
        order(3)
        halo = pltpu.make_async_remote_copy(
            ordered.at[pl.ds(NPOS, SPAN)], ordered.at[pl.ds(0, SPAN)], halo_s, halo_r,
            device_id=(lax.rem(sx + 1, NSX), sy), device_id_type=MESH,
        )
        halo.start()
        order(2)
        order(1)

    with scope("attend0"):
        lax.fori_loop(12 // GROUP, 32 // GROUP, attend, 0)

    with scope("leave0"):
        leave(3)
        leave(2)

    with scope("back0"):
        send_all_back(2, 0)

    with scope("wait_out1"):
        wait_all(arrived.at[pl.ds(0, NDEV - 1), pl.ds(0, 1)], out_s.at[1], out_r.at[1])

    with scope("order1"):
        order(0)
        halo.wait_send()
        halo.wait_recv()
        units(ordered[pl.ds(0, SPAN), :HD].astype(F32), pl.ds(0, SPAN))

    with scope("attend1"):
        lax.fori_loop(0, 12 // GROUP, attend, 0)

    with scope("leave1"):
        leave(1)
        leave(0)

    with scope("back1"):
        send_all_back(0, 1)
        returned[sy, sx] = leaving[me]

    with scope("wait_back0"):
        wait_all(leaving.at[pl.ds(0, NDEV - 1), pl.ds(0, 2)], back_s.at[0], back_r.at[0])
    with scope("wait_back1"):
        wait_all(leaving.at[pl.ds(0, NDEV - 1), pl.ds(0, 2)], back_s.at[1], back_r.at[1])

    with scope("merge"):
        for h in range(HEADS):
            rows = returned[h].astype(F32).reshape(TOK, HD).astype(BF16)
            merged[:, h * HD : (h + 1) * HD] = dot(mergehot[h], rows).astype(BF16)


def per_device(tokens, norm_gain, w_qk, w_value, w_out, send_order, place):
    vmem = pl.BlockSpec(memory_space=pltpu.VMEM)
    hbm = pl.BlockSpec(memory_space=pltpu.HBM)
    dma = pltpu.SemaphoreType.DMA
    merged = pl.pallas_call(
        kernel,
        out_shape=jax.ShapeDtypeStruct((TOK, D), BF16),
        in_specs=[hbm] * 6,
        out_specs=vmem,
        scratch_shapes=[
            pltpu.VMEM((TOK, D), BF16),
            pltpu.VMEM((1, D), F32),
            pltpu.VMEM((D, D), BF16),
            pltpu.VMEM((D, D), BF16),
            pltpu.VMEM((HEADS, TOK), I32),
            pltpu.VMEM((HEADS, TOK), I32),
            pltpu.VMEM((TOK, D), BF16),
            pltpu.VMEM((HEADS, NSX, 4, 8, 2 * HD), BF16),
            pltpu.VMEM((NDEV, 4, 8, 2 * HD), BF16),
            pltpu.VMEM((NDEV, 4, 8, HD), BF16),
            pltpu.VMEM((HEADS, NSX, 4, 8, HD), BF16),
            pltpu.VMEM((HEADS, 1, TOK), I32),
            pltpu.VMEM((NSY, 1, TOK), I32),
            pltpu.VMEM((8, TOK), I32),
            pltpu.VMEM((8, TOK, 128), I32),
            pltpu.VMEM((8, TOK, 128), I32),
            pltpu.VMEM((8, TOK), I32),
            pltpu.VMEM((HEADS, TOK, TOK), BF16),
            pltpu.VMEM((8, TOK, TOK), BF16),
            pltpu.VMEM((8, TOK, TOK), BF16),
            pltpu.VMEM((NPOS + SPAN, 2 * HD), BF16),
            pltpu.VMEM((NPOS + SPAN, HD), BF16),
            pltpu.VMEM((NPOS, HD), BF16),
            dma((6,)),
            pltpu.SemaphoreType.REGULAR,
            dma, dma, dma((2,)), dma((2,)), dma, dma, dma((2,)), dma((2,)),
        ],
        compiler_params=pltpu.CompilerParams(
            collective_id=0, has_side_effects=True, vmem_limit_bytes=VMEM_LIMIT
        ),
    )(*[
        pltpu.with_memory_space_constraint(array, pltpu.HBM)
        for array in (tokens, norm_gain.reshape(1, D), w_qk, w_value, send_order, place)
    ])
    return jnp.dot(merged, w_out, preferred_element_type=F32).astype(BF16)


def solution(mesh):
    return jax.shard_map(
        per_device,
        mesh=mesh,
        in_specs=(P(("sx", "sy"), None), P(), P(), P(), P(), P(None, ("sx", "sy")), P(None, ("sx", "sy"))),
        out_specs=P(("sx", "sy"), None),
        check_vma=False,
    )
```

```python
import random

import jax
import jax.numpy as jnp
from jax import lax
from jax.experimental import pallas as pl
from jax.experimental.pallas import tpu as pltpu
from jax.sharding import PartitionSpec as P

MESH = pl.DeviceIdType.MESH
F32, BF16, I32 = jnp.float32, jnp.bfloat16, jnp.int32
D, HEADS, HD, SPAN, TOK = 1024, 8, 128, 128, 512
NSX, NSY = 16, 8
NDEV = NSX * NSY
NPOS = 8 * TOK
TOGETHER = (15, 8, 9)
PART = 16
EACH = [[(which, part) for part in range(8)] for which in range(3)]
PLAN = [[], [], [], EACH[1], [], [], EACH[2], [], [], []]
VMEM_LIMIT = 44 * 2**20
SCALE = HD ** (-0.5)
LOG2E = 1.4426950408889634
scope = jax.named_scope


GROUPS = [(0, 0), (0, 1), (0, 3), (1, 2), (0, 2), (1, 1), (1, 3), (1, 0)]


def offsets():
    every = [
        (dx, hi, core, lo, dy)
        for dx in range(4) for hi in range(2) for core in range(2) for lo in range(2) for dy in range(4)
    ][1:]
    random.Random(1).shuffle(every)
    every.sort(key=lambda o: -(min(o[0], 4 - o[0]) + min(o[4], 4 - o[4]) + (1 if o[3] else 2 * o[1])))
    return every, [[o for o in every if (o[3], o[4]) == group] for group in GROUPS]


def reach(sx, sy):
    xs = [lax.rem(sx // 4 + d, 4) * 4 for d in range(4)]
    hi, core, lo = lax.rem(sx // 2, 2), lax.rem(sx, 2), sy // 4
    pairs = [[(1 - hi if a else hi) * 2 + (1 - core if b else core) for b in range(2)] for a in range(2)]
    txs = [[[xs[d] + pairs[a][b] for b in range(2)] for a in range(2)] for d in range(4)]
    tys = [[(1 - lo if a else lo) * 4 + lax.rem(lax.rem(sy, 4) + d, 4) for d in range(4)] for a in range(2)]
    return lambda o: (txs[o[0]][o[1]][o[2]], tys[o[3]][o[4]])


def signal(sem, target):
    pl.semaphore_signal(sem, inc=1, device_id=target, device_id_type=MESH)


def swapped(rows):
    lane = lax.broadcasted_iota(I32, rows.shape, 1)
    width = rows.shape[1]
    return jnp.where((lane // 4) % 2 == 0, pltpu.roll(rows, width - 4, 1), pltpu.roll(rows, 4, 1))


def spread(columns, out_ref):
    for j in range(8):
        out_ref[j] = jnp.broadcast_to(columns[:, j : j + 1], (TOK, 128))


def some_rows(columns, first):
    return columns.reshape(NSX, 4, 8, 8)[:, first // 8 : first // 8 + 2].reshape(TOK // 2, 8).T


def hot_rows(column):
    lane = lax.broadcasted_iota(I32, (TOK, 128), 1)
    return jnp.concatenate(
        [jnp.where(column == lane + 128 * c, 1.0, 0.0).astype(BF16) for c in range(TOK // 128)], axis=1
    )


def hot_columns(row):
    token = lax.broadcasted_iota(I32, (TOK, row.shape[1]), 0)
    return jnp.where(token == row, 1.0, 0.0).astype(BF16)


def dot(a, b):
    return jnp.dot(a, b, preferred_element_type=F32)


def halves(first, second):
    low = lax.broadcasted_iota(I32, first.shape, 1) < 4
    return jnp.where(low, first, second)


def kernel(
    tokens_hbm, gain_hbm, wqk_hbm, wv_hbm, send_hbm, place_hbm, merged,
    tokens, gain, weights, send_ref, place_ref, normed, outgoing, arrived, leaving, returned, placeout, placein, placerow,
    placecol, turned, both, sendrow, mergehot, orderhot, leavehot, ordered, unit, sorted_out,
    partial, load_sem, weight_sem, met_sem, place_s, place_r, out_s, out_r, halo_s, halo_r, back_s, back_r,
):
    sx, sy = lax.axis_index("sx"), lax.axis_index("sy")
    me = sx * NSY + sy
    at_offset = reach(sx, sy)
    every, groups = offsets()
    heads = [at_offset((0, 0, 0, *group))[1] for group in GROUPS]

    with scope("signal"):
        barrier = pltpu.get_barrier_semaphore()
        for k in range(1, NSX):
            signal(barrier, (lax.rem(sx + k, NSX), sy))
        for k in range(1, NSY):
            signal(barrier, (sx, lax.rem(sy + k, NSY)))
        loads = [
            pltpu.make_async_copy(src, dst, load_sem.at[n])
            for n, (src, dst) in enumerate([
                (send_hbm, send_ref), (place_hbm, place_ref), (gain_hbm, gain), (tokens_hbm, tokens),
            ])
        ]
        for load in loads:
            load.start()
        weight_loads = []
        for n, h in enumerate(heads):
            columns = pl.ds(pl.multiple_of(h * HD, HD), HD)
            weight_loads.append([
                pltpu.make_async_copy(src.at[:, columns], weights.at[n, :, pl.ds(at, HD)], weight_sem.at[n, at // HD])
                for src, at in ((wqk_hbm, 0), (wv_hbm, HD))
            ])
        for load in weight_loads[0]:
            load.start()

    with scope("index"):
        loads[0].wait()
        for pair in weight_loads[1:]:
            for load in pair:
                load.start()
        for n, h in enumerate(heads):
            turned[n : n + 1, :] = send_ref[pl.ds(h, 1), :]
        odd = lax.rem(sy, 2) == 1
        rows = turned[...]
        columns = jnp.where(odd, swapped(rows), rows).T

    with scope("norm"):
        loads[2].wait()
        loads[3].wait()

        def norm(i, _):
            at = pl.ds(pl.multiple_of(i * 128, 128), 128)
            rows = tokens[at, :].astype(F32)
            stat = jnp.mean(rows * rows, -1, keepdims=True) + 1e-06
            normed[at, :] = (rows * lax.rsqrt(stat) * gain[...]).astype(BF16)
            return 0

        lax.fori_loop(0, TOK // 128, norm, 0)

    def project(n):
        for load in weight_loads[n]:
            load.wait()
        both[n % 2] = dot(normed[...], weights[n]).astype(BF16)

    def permute(n):
        rows = dot(hot_rows(jnp.broadcast_to(columns[:, n : n + 1], (TOK, 128))), both[n % 2])
        outgoing[heads[n]] = rows.reshape(NSX, 4, 8, 2 * HD).astype(BF16)

    def send_rows(first, count, sem, target, sent):
        tx, ty = target
        pltpu.make_async_remote_copy(
            outgoing.at[ty, tx, pl.ds(first, count)],
            arrived.at[me, pl.ds(first, count)],
            out_s.at[sent],
            out_r.at[sem],
            device_id=target,
            device_id_type=MESH,
        ).start()

    with scope("project0"):
        project(0)

    with scope("permute0"):
        project(1)
        permute(0)

    with scope("barrier1"):
        loads[1].wait()
        for h in range(HEADS):
            placeout[h] = place_ref[h : h + 1, :]
        pl.semaphore_wait(barrier, NSX - 1 + NSY - 1)
        for k in range(1, NSY):
            signal(met_sem, (sx, lax.rem(sy + k, NSY)))

    with scope("send_near"):
        for o in groups[0]:
            send_rows(2, 2, 0, at_offset(o), 0)
        for k in range(1, NSY):
            ty = lax.rem(sy + k, NSY)
            pltpu.make_async_remote_copy(
                placeout.at[ty], placein.at[sy], place_s, place_r, device_id=(sx, ty), device_id_type=MESH
            ).start()

    for n in range(1, 8):
        with scope(f"project{n}"):
            if n < 7:
                project(n + 1)
            permute(n)
            if n == 1:
                pl.semaphore_wait(met_sem, NSY - 1)
            for o in groups[n]:
                send_rows(2, 2, 0, at_offset(o), n)

    arrived[me] = outgoing[sy, sx]

    with scope("tables"):
        rows = send_ref[...]
        columns = jnp.where(odd, swapped(rows), rows).T
        for part in range(2):
            sendrow[part] = some_rows(columns, 16 * part)
        def table(h, _):
            for part in range(2):
                mergehot[part, h] = hot_columns(sendrow[part, pl.ds(h, 1), :])
            return 0

        lax.fori_loop(0, HEADS, table, 0)
        whole_place = pltpu.make_async_remote_copy(
            placein.at[pl.ds(0, NSY - 1)], placein.at[pl.ds(0, NSY - 1)], place_s, place_r, device_id=(sx, sy),
            device_id_type=MESH,
        )
        whole_place.wait_send()
        whole_place.wait_recv()
        placein[sy] = placeout[sy]
        for j in range(8):
            placerow[j : j + 1, :] = placein[j]
        block = lax.broadcasted_iota(I32, (8, TOK), 0)
        placerow[...] = jnp.where(block % 2 == 1, swapped(placerow[...]), placerow[...])
        spread(placerow[...].T, placecol)

        def place_table(j, _):
            orderhot[j] = hot_columns(placerow[pl.ds(j, 1), :])
            leavehot[j] = hot_rows(placecol[j])
            return 0

        lax.fori_loop(0, 8, place_table, 0)

    def whole(ref, send_sem, recv_sem):
        return pltpu.make_async_remote_copy(
            ref, ref, send_sem, recv_sem, device_id=(sx, sy), device_id_type=MESH
        )

    def units(keys, at):
        stat = jnp.sum(keys * keys, -1, keepdims=True) + 1e-06
        unit[at, :] = (keys * lax.rsqrt(stat)).astype(BF16)

    def order(q):
        group = arrived[:, q].astype(F32).reshape(NDEV // 2, 2, 8, 2 * HD)
        even, odd = group[:, 0], group[:, 1]
        for b, pair in ((1, (odd, even)), (0, (even, odd))):
            j = 2 * q + b
            mixed = halves(*pair).reshape(TOK, 2 * HD).astype(BF16)
            at = pl.ds(SPAN + j * TOK, TOK)
            rows = dot(orderhot[j], mixed)
            ordered[at, :] = rows.astype(BF16)
            units(rows[:, :HD], at)

    def attend(first, count, together):
        diagonal = lax.broadcasted_iota(I32, (SPAN, SPAN), 0) == lax.broadcasted_iota(I32, (SPAN, SPAN), 1)

        def some(g, _):
            for u in range(together):
                c = first + g * together + u
                at = pl.ds(pl.multiple_of(c * SPAN, SPAN), 2 * SPAN)
                query = ordered[pl.ds(pl.multiple_of(c * SPAN + SPAN, SPAN), SPAN), :HD]
                scores = lax.dot_general(query, unit[at, :], (((1,), (1,)), ((), ())), preferred_element_type=F32)
                before, own = scores[:, :SPAN], jnp.where(diagonal, -100000.0 / SCALE, scores[:, SPAN:])
                peak = jnp.max(jnp.maximum(before, own), -1, keepdims=True)
                before, own = jnp.exp2((before - peak) * (SCALE * LOG2E)), jnp.exp2((own - peak) * (SCALE * LOG2E))
                share = 1.0 / jnp.sum(before + own, -1, keepdims=True)
                shares = jnp.concatenate([before * share, own * share], axis=1).astype(BF16)
                sorted_out[pl.ds(pl.multiple_of(c * SPAN, SPAN), SPAN), :] = dot(shares, ordered[at, HD:]).astype(BF16)
            return 0

        lax.fori_loop(0, count // together, some, 0)

    def leave(q):
        parts = []
        for b in range(2):
            j = q * 2 + b
            rows = sorted_out[pl.ds(j * TOK, TOK), :]
            parts.append(dot(leavehot[j], rows).reshape(NDEV // 2, 8, HD))
        pair = jnp.stack([halves(parts[0], parts[1]), halves(parts[1], parts[0])], axis=1)
        leaving[:, q] = pair.reshape(NDEV, 8, HD).astype(BF16)

    def send_back(first, count, target, sem):
        tx, ty = target
        pltpu.make_async_remote_copy(
            leaving.at[tx * NSY + ty, pl.ds(first, count)],
            returned.at[sy, sx, pl.ds(first, count)],
            back_s.at[sem],
            back_r.at[sem],
            device_id=target,
            device_id_type=MESH,
        ).start()

    def came(first, count, sem):
        whole(arrived.at[pl.ds(0, NDEV - 1), pl.ds(first, count)], out_s.at[0], out_r.at[sem]).wait_recv()

    def left(n, count, messages):
        whole(arrived.at[pl.ds(0, messages), pl.ds(0, count)], out_s.at[n], out_r.at[0]).wait_send()

    def parts_of(n):
        return every[n * PART : (n + 1) * PART]

    def send_part(which, n):
        for o in parts_of(n):
            send_rows(2 - which, 1, which, at_offset(o), 8 * which + n)

    with scope("send_out1"):
        for n in range(8):
            left(n, 2, len(groups[n]))
            for which, part in PLAN[n]:
                send_part(which, part)

    with scope("wait_out0"):
        came(2, 2, 0)

    with scope("order0"):
        order(3)
        halo = pltpu.make_async_remote_copy(
            ordered.at[pl.ds(NPOS, SPAN)], ordered.at[pl.ds(0, SPAN)], halo_s, halo_r,
            device_id=(lax.rem(sx + 1, NSX), sy), device_id_type=MESH,
        )
        halo.start()
        order(2)

    with scope("attend0"):
        for which, part in PLAN[8]:
            send_part(which, part)
        attend(17, 15, TOGETHER[0])
        for which, part in PLAN[9]:
            send_part(which, part)

    with scope("leave0"):
        leave(3)

    with scope("back0"):
        for o in every:
            send_back(3, 1, at_offset(o), 0)

    with scope("wait_out1"):
        came(1, 1, 1)

    with scope("order1"):
        order(1)

    with scope("attend1"):
        attend(9, 8, TOGETHER[1])

    with scope("leave1"):
        leave(2)

    with scope("back1"):
        for o in every:
            send_back(2, 1, at_offset(o), 1)

    with scope("wait_out2"):
        came(0, 1, 2)
        for n in range(8, 24):
            left(n, 1, len(parts_of(n % 8)))

    with scope("order2"):
        order(0)
        halo.wait_send()
        halo.wait_recv()
        units(ordered[pl.ds(0, SPAN), :HD].astype(F32), pl.ds(0, SPAN))

    with scope("attend2"):
        attend(0, 9, TOGETHER[2])

    with scope("leave2"):
        leave(1)
        leave(0)

    with scope("back2"):
        for o in every:
            send_back(0, 2, at_offset(o), 2)
        returned[sy, sx] = leaving[me]

    def merge(part, h):
        rows = returned[h, :, pl.ds(2 * part, 2)].astype(F32).reshape(TOK // 2, HD).astype(BF16)
        return dot(mergehot[part, h], rows)

    with scope("wait_back0"):
        for n in range(2):
            back = whole(leaving.at[pl.ds(0, NDEV - 1), pl.ds(0, 1)], back_s.at[n], back_r.at[n])
            back.wait_send()
            back.wait_recv()

    with scope("merge0"):
        for h in range(HEADS):
            partial[h] = merge(1, h)

    with scope("wait_back2"):
        back = whole(leaving.at[pl.ds(0, NDEV - 1), pl.ds(0, 2)], back_s.at[2], back_r.at[2])
        back.wait_send()
        back.wait_recv()

    with scope("merge"):
        for h in range(HEADS):
            merged[:, h * HD : (h + 1) * HD] = (partial[h] + merge(0, h)).astype(BF16)


def per_device(tokens, norm_gain, w_qk, w_value, w_out, send_order, place):
    vmem = pl.BlockSpec(memory_space=pltpu.VMEM)
    hbm = pl.BlockSpec(memory_space=pltpu.HBM)
    dma = pltpu.SemaphoreType.DMA
    merged = pl.pallas_call(
        kernel,
        out_shape=jax.ShapeDtypeStruct((TOK, D), BF16),
        in_specs=[hbm] * 6,
        out_specs=vmem,
        scratch_shapes=[
            pltpu.VMEM((TOK, D), BF16),
            pltpu.VMEM((1, D), F32),
            pltpu.VMEM((HEADS, D, 2 * HD), BF16),
            pltpu.VMEM((HEADS, TOK), I32),
            pltpu.VMEM((HEADS, TOK), I32),
            pltpu.VMEM((TOK, D), BF16),
            pltpu.VMEM((HEADS, NSX, 4, 8, 2 * HD), BF16),
            pltpu.VMEM((NDEV, 4, 8, 2 * HD), BF16),
            pltpu.VMEM((NDEV, 4, 8, HD), BF16),
            pltpu.VMEM((HEADS, NSX, 4, 8, HD), BF16),
            pltpu.VMEM((HEADS, 1, TOK), I32),
            pltpu.VMEM((NSY, 1, TOK), I32),
            pltpu.VMEM((8, TOK), I32),
            pltpu.VMEM((8, TOK, 128), I32),
            pltpu.VMEM((8, TOK), I32),
            pltpu.VMEM((2, TOK, 2 * HD), BF16),
            pltpu.VMEM((2, 8, TOK // 2), I32),
            pltpu.VMEM((2, HEADS, TOK, TOK // 2), BF16),
            pltpu.VMEM((8, TOK, TOK), BF16),
            pltpu.VMEM((8, TOK, TOK), BF16),
            pltpu.VMEM((NPOS + SPAN, 2 * HD), BF16),
            pltpu.VMEM((NPOS + SPAN, HD), BF16),
            pltpu.VMEM((NPOS, HD), BF16),
            pltpu.VMEM((HEADS, TOK, HD), F32),
            dma((4,)),
            dma((HEADS, 2)),
            pltpu.SemaphoreType.REGULAR,
            dma, dma, dma((24,)), dma((3,)), dma, dma, dma((3,)), dma((3,)),
        ],
        compiler_params=pltpu.CompilerParams(
            collective_id=0, has_side_effects=True, vmem_limit_bytes=VMEM_LIMIT
        ),
    )(*[
        pltpu.with_memory_space_constraint(array, pltpu.HBM)
        for array in (tokens, norm_gain.reshape(1, D), w_qk, w_value, send_order, place)
    ])
    return jnp.dot(merged, w_out, preferred_element_type=F32).astype(BF16)


def solution(mesh):
    return jax.shard_map(
        per_device,
        mesh=mesh,
        in_specs=(P(("sx", "sy"), None), P(), P(), P(), P(), P(None, ("sx", "sy")), P(None, ("sx", "sy"))),
        out_specs=P(("sx", "sy"), None),
        check_vma=False,
    )
```

```python
import random

import jax
import jax.numpy as jnp
from jax import lax
from jax.experimental import pallas as pl
from jax.experimental.pallas import tpu as pltpu
from jax.sharding import PartitionSpec as P

MESH = pl.DeviceIdType.MESH
F32, BF16, I32 = jnp.float32, jnp.bfloat16, jnp.int32
D, HEADS, HD, SPAN, TOK = 1024, 8, 128, 128, 512
NSX, NSY = 16, 8
NDEV = NSX * NSY
NPOS = 8 * TOK
BATCHES = [(1, 2), (3, 4), (5, 6, 7)]
VMEM_LIMIT = 44 * 2**20
SCALE = HD ** (-0.5)
LOG2E = 1.4426950408889634
scope = jax.named_scope


GROUPS = [(0, 0), (0, 1), (0, 3), (1, 2), (0, 2), (1, 1), (1, 3), (1, 0)]


def offsets():
    every = [
        (dx, hi, core, lo, dy)
        for dx in range(4) for hi in range(2) for core in range(2) for lo in range(2) for dy in range(4)
    ][1:]
    random.Random(1).shuffle(every)
    every.sort(key=lambda o: -(min(o[0], 4 - o[0]) + min(o[4], 4 - o[4]) + (1 if o[3] else 2 * o[1])))
    return every, [[o for o in every if (o[3], o[4]) == group] for group in GROUPS]


def reach(sx, sy):
    xs = [lax.rem(sx // 4 + d, 4) * 4 for d in range(4)]
    hi, core, lo = lax.rem(sx // 2, 2), lax.rem(sx, 2), sy // 4
    pairs = [[(1 - hi if a else hi) * 2 + (1 - core if b else core) for b in range(2)] for a in range(2)]
    txs = [[[xs[d] + pairs[a][b] for b in range(2)] for a in range(2)] for d in range(4)]
    tys = [[(1 - lo if a else lo) * 4 + lax.rem(lax.rem(sy, 4) + d, 4) for d in range(4)] for a in range(2)]
    return lambda o: (txs[o[0]][o[1]][o[2]], tys[o[3]][o[4]])


def signal(sem, target):
    pl.semaphore_signal(sem, inc=1, device_id=target, device_id_type=MESH)


def swapped(rows):
    lane = lax.broadcasted_iota(I32, rows.shape, 1)
    width = rows.shape[1]
    return jnp.where((lane // 4) % 2 == 0, pltpu.roll(rows, width - 4, 1), pltpu.roll(rows, 4, 1))


def spread(columns, out_ref):
    for j in range(8):
        out_ref[j] = jnp.broadcast_to(columns[:, j : j + 1], (TOK, 128))


def some_rows(columns, q):
    return columns.reshape(NSX, 4, 8, 8)[:, q].reshape(TOK // 4, 8).T


def hot_rows(column):
    lane = lax.broadcasted_iota(I32, (TOK, 128), 1)
    return jnp.concatenate(
        [jnp.where(column == lane + 128 * c, 1.0, 0.0).astype(BF16) for c in range(TOK // 128)], axis=1
    )


def hot_columns(row):
    token = lax.broadcasted_iota(I32, (TOK, row.shape[1]), 0)
    return jnp.where(token == row, 1.0, 0.0).astype(BF16)


def dot(a, b):
    return jnp.dot(a, b, preferred_element_type=F32)


def halves(first, second):
    low = lax.broadcasted_iota(I32, first.shape, 1) < 4
    return jnp.where(low, first, second)


def kernel(
    tokens_hbm, gain_hbm, wqk_hbm, wv_hbm, send_hbm, place_hbm, merged,
    tokens, gain, weights, send_ref, place_ref, normed, outgoing, arrived, leaving, returned, placeout, placein, placerow,
    placecol, turned, both, sendrow, mergehot, orderhot, leavehot, ordered, unit, sorted_out,
    partial, load_sem, weight_sem, met_sem, place_s, place_r, out_s, out_r, halo_s, halo_r, back_s, back_r,
):
    sx, sy = lax.axis_index("sx"), lax.axis_index("sy")
    me = sx * NSY + sy
    at_offset = reach(sx, sy)
    every, groups = offsets()
    heads = [at_offset((0, 0, 0, *group))[1] for group in GROUPS]

    with scope("signal"):
        barrier = pltpu.get_barrier_semaphore()
        for k in range(1, NSX):
            signal(barrier, (lax.rem(sx + k, NSX), sy))
        for k in range(1, NSY):
            signal(barrier, (sx, lax.rem(sy + k, NSY)))
        loads = [
            pltpu.make_async_copy(src, dst, load_sem.at[n])
            for n, (src, dst) in enumerate([
                (send_hbm, send_ref), (place_hbm, place_ref), (gain_hbm, gain),
                *[(tokens_hbm.at[pl.ds(i, 128)], tokens.at[pl.ds(i, 128)]) for i in range(0, TOK, 128)],
            ])
        ]
        for load in loads:
            load.start()
        weight_loads = []
        for n, h in enumerate(heads):
            columns = pl.ds(pl.multiple_of(h * HD, HD), HD)
            weight_loads.append([
                pltpu.make_async_copy(src.at[:, columns], weights.at[n, :, pl.ds(at, HD)], weight_sem.at[n, at // HD])
                for src, at in ((wqk_hbm, 0), (wv_hbm, HD))
            ])
        for load in weight_loads[0]:
            load.start()

    with scope("index"):
        loads[0].wait()
        for pair in weight_loads[1:]:
            for load in pair:
                load.start()
        for n, h in enumerate(heads):
            turned[n : n + 1, :] = send_ref[pl.ds(h, 1), :]
        odd = lax.rem(sy, 2) == 1
        rows = turned[...]
        columns = jnp.where(odd, swapped(rows), rows).T

    with scope("norm"):
        loads[2].wait()
        for i in range(4):
            loads[3 + i].wait()
            rows = tokens[128 * i : 128 * i + 128, :].astype(F32)
            stat = jnp.mean(rows * rows, -1, keepdims=True) + 1e-06
            normed[128 * i : 128 * i + 128, :] = (rows * lax.rsqrt(stat) * gain[...]).astype(BF16)

    def project(n):
        for load in weight_loads[n]:
            load.wait()
        both[n % 2] = dot(normed[...], weights[n]).astype(BF16)

    def permute(n):
        rows = dot(hot_rows(jnp.broadcast_to(columns[:, n : n + 1], (TOK, 128))), both[n % 2])
        outgoing[heads[n]] = rows.reshape(NSX, 4, 8, 2 * HD).astype(BF16)

    def send_rows(first, count, which, target):
        tx, ty = target
        pltpu.make_async_remote_copy(
            outgoing.at[ty, tx, pl.ds(first, count)],
            arrived.at[me, pl.ds(first, count)],
            out_s.at[which],
            out_r.at[which],
            device_id=target,
            device_id_type=MESH,
        ).start()

    with scope("project0"):
        project(0)

    with scope("permute0"):
        project(1)
        permute(0)

    with scope("barrier1"):
        loads[1].wait()
        for h in range(HEADS):
            placeout[h] = place_ref[h : h + 1, :]
        pl.semaphore_wait(barrier, NSX - 1 + NSY - 1)
        for k in range(1, NSY):
            signal(met_sem, (sx, lax.rem(sy + k, NSY)))

    with scope("send_near"):
        for o in groups[0]:
            send_rows(2, 2, 0, at_offset(o))
        for k in range(1, NSY):
            ty = lax.rem(sy + k, NSY)
            pltpu.make_async_remote_copy(
                placeout.at[ty], placein.at[sy], place_s, place_r, device_id=(sx, ty), device_id_type=MESH
            ).start()

    for batch in BATCHES:
        with scope(f"project{batch[0]}"):
            for n in batch:
                if n < 7:
                    project(n + 1)
                permute(n)
        with scope(f"send{batch[0]}"):
            if batch[0] == 1:
                pl.semaphore_wait(met_sem, NSY - 1)
            for o in every:
                n = GROUPS.index(o[3:])
                if n in batch:
                    send_rows(2, 2, 0, at_offset(o))

    arrived[me] = outgoing[sy, sx]

    def whole(ref, send_sem, recv_sem):
        return pltpu.make_async_remote_copy(
            ref, ref, send_sem, recv_sem, device_id=(sx, sy), device_id_type=MESH
        )

    with scope("send_rest"):
        for which in (1, 2):
            for o in every:
                send_rows(2 - which, 1, which, at_offset(o))

    def came(which):
        out = whole(arrived.at[pl.ds(0, NDEV - 1), pl.ds(0, (2, 1, 1)[which])], out_s.at[which], out_r.at[which])
        out.wait_send()
        out.wait_recv()

    with scope("tables"):
        rows = send_ref[...]
        columns = jnp.where(odd, swapped(rows), rows).T
        for q in range(4):
            sendrow[q] = some_rows(columns, q)
        def table(h, _):
            for q in range(4):
                mergehot[q, h] = hot_columns(sendrow[q, pl.ds(h, 1), :])
            return 0

        lax.fori_loop(0, HEADS, table, 0)
        whole_place = pltpu.make_async_remote_copy(
            placein.at[pl.ds(0, NSY - 1)], placein.at[pl.ds(0, NSY - 1)], place_s, place_r, device_id=(sx, sy),
            device_id_type=MESH,
        )
        whole_place.wait_send()
        whole_place.wait_recv()
        placein[sy] = placeout[sy]
        for j in range(8):
            placerow[j : j + 1, :] = placein[j]
        block = lax.broadcasted_iota(I32, (8, TOK), 0)
        placerow[...] = jnp.where(block % 2 == 1, swapped(placerow[...]), placerow[...])
        spread(placerow[...].T, placecol)

        def place_table(j, _):
            orderhot[j] = hot_columns(placerow[pl.ds(j, 1), :])
            leavehot[j] = hot_rows(placecol[j])
            return 0

        lax.fori_loop(0, 8, place_table, 0)

    def units(keys, at):
        stat = jnp.sum(keys * keys, -1, keepdims=True) + 1e-06
        unit[at, :] = (keys * lax.rsqrt(stat)).astype(BF16)

    def order(q, b):
        group = arrived[:, q].astype(F32).reshape(NDEV // 2, 2, 8, 2 * HD)
        even, odd = group[:, 0], group[:, 1]
        j = 2 * q + b
        mixed = (halves(odd, even) if b else halves(even, odd)).reshape(TOK, 2 * HD).astype(BF16)
        at = pl.ds(SPAN + j * TOK, TOK)
        rows = dot(orderhot[j], mixed)
        ordered[at, :] = rows.astype(BF16)
        units(rows[:, :HD], at)

    def attend(first, count):
        diagonal = lax.broadcasted_iota(I32, (SPAN, SPAN), 0) == lax.broadcasted_iota(I32, (SPAN, SPAN), 1)
        for c in range(first, first + count):
            at = pl.ds(c * SPAN, 2 * SPAN)
            query = ordered[pl.ds(c * SPAN + SPAN, SPAN), :HD]
            scores = lax.dot_general(query, unit[at, :], (((1,), (1,)), ((), ())), preferred_element_type=F32)
            before, own = scores[:, :SPAN], jnp.where(diagonal, -100000.0 / SCALE, scores[:, SPAN:])
            peak = jnp.max(jnp.maximum(before, own), -1, keepdims=True)
            before, own = jnp.exp2((before - peak) * (SCALE * LOG2E)), jnp.exp2((own - peak) * (SCALE * LOG2E))
            share = 1.0 / jnp.sum(before + own, -1, keepdims=True)
            shares = jnp.concatenate([before * share, own * share], axis=1).astype(BF16)
            sorted_out[pl.ds(c * SPAN, SPAN), :] = dot(shares, ordered[at, HD:]).astype(BF16)

    def leave(q):
        parts = []
        for b in range(2):
            j = q * 2 + b
            rows = sorted_out[pl.ds(j * TOK, TOK), :]
            parts.append(dot(leavehot[j], rows).reshape(NDEV // 2, 8, HD))
        pair = jnp.stack([halves(parts[0], parts[1]), halves(parts[1], parts[0])], axis=1)
        leaving[:, q] = pair.reshape(NDEV, 8, HD).astype(BF16)

    def send_back(q):
        for o in every:
            tx, ty = at_offset(o)
            pltpu.make_async_remote_copy(
                leaving.at[tx * NSY + ty, q],
                returned.at[sy, sx, q],
                back_s.at[q],
                back_r.at[q],
                device_id=(tx, ty),
                device_id_type=MESH,
            ).start()
        returned[sy, sx, q] = leaving[me, q]

    def returns(q):
        back = whole(leaving.at[pl.ds(0, NDEV - 1), 0], back_s.at[q], back_r.at[q])
        back.wait_send()
        back.wait_recv()

    def merge(q, h):
        rows = returned[h, :, q].astype(F32).reshape(TOK // 4, HD).astype(BF16)
        return dot(mergehot[q, h], rows)

    with scope("wait_out0"):
        came(0)

    with scope("order0"):
        order(3, 1)
        order(3, 0)
        halo = pltpu.make_async_remote_copy(
            ordered.at[pl.ds(NPOS, SPAN)], ordered.at[pl.ds(0, SPAN)], halo_s, halo_r,
            device_id=(lax.rem(sx + 1, NSX), sy), device_id_type=MESH,
        )
        halo.start()
        order(2, 1)
        order(2, 0)

    with scope("attend0"):
        attend(17, 15)

    with scope("leave0"):
        leave(3)

    with scope("back0"):
        send_back(3)

    with scope("wait_out1"):
        came(1)

    with scope("order1"):
        order(1, 1)
        order(1, 0)

    with scope("attend1"):
        attend(9, 8)

    with scope("leave1"):
        leave(2)

    with scope("back1"):
        send_back(2)

    with scope("wait_out2"):
        came(2)

    with scope("order2"):
        order(0, 1)

    with scope("attend2"):
        attend(8, 1)

    with scope("leave2"):
        leave(1)

    with scope("back2"):
        send_back(1)

    with scope("order3"):
        order(0, 0)
        halo.wait_send()
        halo.wait_recv()
        units(ordered[pl.ds(0, SPAN), :HD].astype(F32), pl.ds(0, SPAN))

    with scope("attend3"):
        attend(0, 8)

    with scope("leave3"):
        leave(0)

    with scope("back3"):
        send_back(0)

    for q in (3, 2, 1):
        with scope(f"wait_back{q}"):
            returns(q)
        with scope(f"merge{q}"):
            for h in range(HEADS):
                partial[h] = merge(q, h) if q == 3 else partial[h] + merge(q, h)

    with scope("wait_back0"):
        returns(0)

    with scope("merge"):
        for h in range(HEADS):
            merged[:, h * HD : (h + 1) * HD] = (partial[h] + merge(0, h)).astype(BF16)


def per_device(tokens, norm_gain, w_qk, w_value, w_out, send_order, place):
    vmem = pl.BlockSpec(memory_space=pltpu.VMEM)
    hbm = pl.BlockSpec(memory_space=pltpu.HBM)
    dma = pltpu.SemaphoreType.DMA
    merged = pl.pallas_call(
        kernel,
        out_shape=jax.ShapeDtypeStruct((TOK, D), BF16),
        in_specs=[hbm] * 6,
        out_specs=vmem,
        scratch_shapes=[
            pltpu.VMEM((TOK, D), BF16),
            pltpu.VMEM((1, D), F32),
            pltpu.VMEM((HEADS, D, 2 * HD), BF16),
            pltpu.VMEM((HEADS, TOK), I32),
            pltpu.VMEM((HEADS, TOK), I32),
            pltpu.VMEM((TOK, D), BF16),
            pltpu.VMEM((HEADS, NSX, 4, 8, 2 * HD), BF16),
            pltpu.VMEM((NDEV, 4, 8, 2 * HD), BF16),
            pltpu.VMEM((NDEV, 4, 8, HD), BF16),
            pltpu.VMEM((HEADS, NSX, 4, 8, HD), BF16),
            pltpu.VMEM((HEADS, 1, TOK), I32),
            pltpu.VMEM((NSY, 1, TOK), I32),
            pltpu.VMEM((8, TOK), I32),
            pltpu.VMEM((8, TOK, 128), I32),
            pltpu.VMEM((8, TOK), I32),
            pltpu.VMEM((2, TOK, 2 * HD), BF16),
            pltpu.VMEM((4, 8, TOK // 4), I32),
            pltpu.VMEM((4, HEADS, TOK, TOK // 4), BF16),
            pltpu.VMEM((8, TOK, TOK), BF16),
            pltpu.VMEM((8, TOK, TOK), BF16),
            pltpu.VMEM((NPOS + SPAN, 2 * HD), BF16),
            pltpu.VMEM((NPOS + SPAN, HD), BF16),
            pltpu.VMEM((NPOS, HD), BF16),
            pltpu.VMEM((HEADS, TOK, HD), F32),
            dma((7,)),
            dma((HEADS, 2)),
            pltpu.SemaphoreType.REGULAR,
            dma, dma, dma((3,)), dma((3,)), dma, dma, dma((4,)), dma((4,)),
        ],
        compiler_params=pltpu.CompilerParams(
            collective_id=0, has_side_effects=True, vmem_limit_bytes=VMEM_LIMIT
        ),
    )(*[
        pltpu.with_memory_space_constraint(array, pltpu.HBM)
        for array in (tokens, norm_gain.reshape(1, D), w_qk, w_value, send_order, place)
    ])
    return jnp.dot(merged, w_out, preferred_element_type=F32).astype(BF16)


def solution(mesh):
    return jax.shard_map(
        per_device,
        mesh=mesh,
        in_specs=(P(("sx", "sy"), None), P(), P(), P(), P(), P(None, ("sx", "sy")), P(None, ("sx", "sy"))),
        out_specs=P(("sx", "sy"), None),
        check_vma=False,
    )
```

```python
import random

import jax
import jax.numpy as jnp
from jax import lax
from jax.experimental import pallas as pl
from jax.experimental.pallas import tpu as pltpu
from jax.sharding import PartitionSpec as P

MESH = pl.DeviceIdType.MESH
F32, BF16, I32 = jnp.float32, jnp.bfloat16, jnp.int32
D, HEADS, HD, SPAN, TOK = 1024, 8, 128, 128, 512
NSX, NSY = 16, 8
NDEV = NSX * NSY
NPOS = 8 * TOK
BATCHES = [(1, 2), (3, 4), (5, 6, 7)]
VMEM_LIMIT = 44 * 2**20
SCALE = HD ** (-0.5)
LOG2E = 1.4426950408889634
scope = jax.named_scope


GROUPS = [(0, 0), (0, 1), (0, 3), (1, 2), (0, 2), (1, 1), (1, 3), (1, 0)]


def offsets():
    every = [
        (dx, hi, core, lo, dy)
        for dx in range(4) for hi in range(2) for core in range(2) for lo in range(2) for dy in range(4)
    ][1:]
    random.Random(1).shuffle(every)
    every.sort(key=lambda o: -(min(o[0], 4 - o[0]) + min(o[4], 4 - o[4]) + (1 if o[3] else 2 * o[1])))
    return every, [[o for o in every if (o[3], o[4]) == group] for group in GROUPS]


def reach(sx, sy):
    xs = [lax.rem(sx // 4 + d, 4) * 4 for d in range(4)]
    hi, core, lo = lax.rem(sx // 2, 2), lax.rem(sx, 2), sy // 4
    pairs = [[(1 - hi if a else hi) * 2 + (1 - core if b else core) for b in range(2)] for a in range(2)]
    txs = [[[xs[d] + pairs[a][b] for b in range(2)] for a in range(2)] for d in range(4)]
    tys = [[(1 - lo if a else lo) * 4 + lax.rem(lax.rem(sy, 4) + d, 4) for d in range(4)] for a in range(2)]
    return lambda o: (txs[o[0]][o[1]][o[2]], tys[o[3]][o[4]])


def signal(sem, target):
    pl.semaphore_signal(sem, inc=1, device_id=target, device_id_type=MESH)


def swapped(rows):
    lane = lax.broadcasted_iota(I32, rows.shape, 1)
    width = rows.shape[1]
    return jnp.where((lane // 4) % 2 == 0, pltpu.roll(rows, width - 4, 1), pltpu.roll(rows, 4, 1))


def spread(columns, out_ref):
    for j in range(8):
        out_ref[j] = jnp.broadcast_to(columns[:, j : j + 1], (TOK, 128))


def some_rows(columns, q):
    return columns.reshape(NSX, 4, 8, 8)[:, q].reshape(TOK // 4, 8).T


def hot_rows(column):
    lane = lax.broadcasted_iota(I32, (TOK, 128), 1)
    return jnp.concatenate(
        [jnp.where(column == lane + 128 * c, 1.0, 0.0).astype(BF16) for c in range(TOK // 128)], axis=1
    )


def hot_columns(row):
    token = lax.broadcasted_iota(I32, (TOK, row.shape[1]), 0)
    return jnp.where(token == row, 1.0, 0.0).astype(BF16)


def dot(a, b):
    return jnp.dot(a, b, preferred_element_type=F32)


def halves(first, second):
    low = lax.broadcasted_iota(I32, first.shape, 1) < 4
    return jnp.where(low, first, second)


def kernel(
    tokens_hbm, gain_hbm, wqk_hbm, wv_hbm, send_hbm, place_hbm, merged,
    tokens, gain, weights, send_ref, place_ref, normed, outgoing, arrived, leaving, returned, placeout, placein, placerow,
    placecol, turned, both, sendrow, mergehot, orderhot, leavehot, ordered, unit, sorted_out,
    partial, load_sem, weight_sem, met_sem, place_s, place_r, out_s, out_r, halo_s, halo_r, back_s, back_r,
):
    sx, sy = lax.axis_index("sx"), lax.axis_index("sy")
    me = sx * NSY + sy
    at_offset = reach(sx, sy)
    every, groups = offsets()
    heads = [at_offset((0, 0, 0, *group))[1] for group in GROUPS]

    with scope("signal"):
        barrier = pltpu.get_barrier_semaphore()
        for k in range(1, NSX):
            signal(barrier, (lax.rem(sx + k, NSX), sy))
        for k in range(1, NSY):
            signal(barrier, (sx, lax.rem(sy + k, NSY)))
        loads = [
            pltpu.make_async_copy(src, dst, load_sem.at[n])
            for n, (src, dst) in enumerate([
                (send_hbm, send_ref), (place_hbm, place_ref), (gain_hbm, gain),
                *[(tokens_hbm.at[pl.ds(i, 128)], tokens.at[pl.ds(i, 128)]) for i in range(0, TOK, 128)],
            ])
        ]
        for load in loads:
            load.start()
        weight_loads = []
        for n, h in enumerate(heads):
            columns = pl.ds(pl.multiple_of(h * HD, HD), HD)
            weight_loads.append([
                pltpu.make_async_copy(src.at[:, columns], weights.at[n, :, pl.ds(at, HD)], weight_sem.at[n, at // HD])
                for src, at in ((wqk_hbm, 0), (wv_hbm, HD))
            ])
        for load in weight_loads[0]:
            load.start()

    with scope("index"):
        loads[0].wait()
        for pair in weight_loads[1:]:
            for load in pair:
                load.start()
        for n, h in enumerate(heads):
            turned[n : n + 1, :] = send_ref[pl.ds(h, 1), :]
        odd = lax.rem(sy, 2) == 1
        rows = turned[...]
        columns = jnp.where(odd, swapped(rows), rows).T

    with scope("norm"):
        loads[2].wait()
        for i in range(4):
            loads[3 + i].wait()
            rows = tokens[128 * i : 128 * i + 128, :].astype(F32)
            stat = jnp.mean(rows * rows, -1, keepdims=True) + 1e-06
            normed[128 * i : 128 * i + 128, :] = (rows * lax.rsqrt(stat) * gain[...]).astype(BF16)

    def project(n):
        for load in weight_loads[n]:
            load.wait()
        both[n % 2] = dot(normed[...], weights[n]).astype(BF16)

    def permute(n):
        rows = dot(hot_rows(jnp.broadcast_to(columns[:, n : n + 1], (TOK, 128))), both[n % 2])
        outgoing[heads[n]] = rows.reshape(NSX, 4, 8, 2 * HD).astype(BF16)

    def send_rows(first, count, which, target):
        tx, ty = target
        pltpu.make_async_remote_copy(
            outgoing.at[ty, tx, pl.ds(first, count)],
            arrived.at[me, pl.ds(first, count)],
            out_s.at[which],
            out_r.at[which],
            device_id=target,
            device_id_type=MESH,
        ).start()

    with scope("project0"):
        project(0)

    with scope("permute0"):
        project(1)
        permute(0)

    with scope("barrier1"):
        loads[1].wait()
        for h in range(HEADS):
            placeout[h] = place_ref[h : h + 1, :]
        pl.semaphore_wait(barrier, NSX - 1 + NSY - 1)
        for k in range(1, NSY):
            signal(met_sem, (sx, lax.rem(sy + k, NSY)))

    with scope("send_near"):
        for o in groups[0]:
            send_rows(2, 2, 0, at_offset(o))
        for k in range(1, NSY):
            ty = lax.rem(sy + k, NSY)
            pltpu.make_async_remote_copy(
                placeout.at[ty], placein.at[sy], place_s, place_r, device_id=(sx, ty), device_id_type=MESH
            ).start()

    for batch in BATCHES:
        with scope(f"project{batch[0]}"):
            for n in batch:
                if n < 7:
                    project(n + 1)
                permute(n)
        with scope(f"send{batch[0]}"):
            if batch[0] == 1:
                pl.semaphore_wait(met_sem, NSY - 1)
            for o in every:
                n = GROUPS.index(o[3:])
                if n in batch:
                    send_rows(2, 2, 0, at_offset(o))

    arrived[me] = outgoing[sy, sx]

    def whole(ref, send_sem, recv_sem):
        return pltpu.make_async_remote_copy(
            ref, ref, send_sem, recv_sem, device_id=(sx, sy), device_id_type=MESH
        )

    with scope("send_rest"):
        for which in (1, 2):
            for o in every:
                send_rows(2 - which, 1, which, at_offset(o))

    def came(which):
        out = whole(arrived.at[pl.ds(0, NDEV - 1), pl.ds(0, (2, 1, 1)[which])], out_s.at[which], out_r.at[which])
        out.wait_send()
        out.wait_recv()

    with scope("tables"):
        rows = send_ref[...]
        columns = jnp.where(odd, swapped(rows), rows).T
        for q in range(4):
            sendrow[q] = some_rows(columns, q)
        def table(h, _):
            for q in range(4):
                mergehot[q, h] = hot_columns(sendrow[q, pl.ds(h, 1), :])
            return 0

        lax.fori_loop(0, HEADS, table, 0)
        whole_place = pltpu.make_async_remote_copy(
            placein.at[pl.ds(0, NSY - 1)], placein.at[pl.ds(0, NSY - 1)], place_s, place_r, device_id=(sx, sy),
            device_id_type=MESH,
        )
        whole_place.wait_send()
        whole_place.wait_recv()
        placein[sy] = placeout[sy]
        for j in range(8):
            placerow[j : j + 1, :] = placein[j]
        block = lax.broadcasted_iota(I32, (8, TOK), 0)
        placerow[...] = jnp.where(block % 2 == 1, swapped(placerow[...]), placerow[...])
        spread(placerow[...].T, placecol)

        def place_table(j, _):
            orderhot[j] = hot_columns(placerow[pl.ds(j, 1), :])
            leavehot[j] = hot_rows(placecol[j])
            return 0

        lax.fori_loop(0, 8, place_table, 0)

    def units(keys, at):
        stat = jnp.sum(keys * keys, -1, keepdims=True) + 1e-06
        unit[at, :] = (keys * lax.rsqrt(stat)).astype(BF16)

    def order(q, b):
        group = arrived[pl.ds(0, NDEV), q].astype(F32).reshape(NDEV // 2, 2, 8, 2 * HD)
        even, odd = group[:, 0], group[:, 1]
        j = 2 * q + b
        mixed = (halves(odd, even) if b else halves(even, odd)).reshape(TOK, 2 * HD).astype(BF16)
        at = pl.ds(SPAN + j * TOK, TOK)
        rows = dot(orderhot[j], mixed)
        ordered[at, :] = rows.astype(BF16)
        units(rows[:, :HD], at)

    def attend(first, count):
        diagonal = lax.broadcasted_iota(I32, (SPAN, SPAN), 0) == lax.broadcasted_iota(I32, (SPAN, SPAN), 1)
        for c in range(first, first + count):
            at = pl.ds(c * SPAN, 2 * SPAN)
            query = ordered[pl.ds(c * SPAN + SPAN, SPAN), :HD]
            scores = lax.dot_general(query, unit[at, :], (((1,), (1,)), ((), ())), preferred_element_type=F32)
            before, own = scores[:, :SPAN], jnp.where(diagonal, -100000.0 / SCALE, scores[:, SPAN:])
            peak = jnp.max(jnp.maximum(before, own), -1, keepdims=True)
            before, own = jnp.exp2((before - peak) * (SCALE * LOG2E)), jnp.exp2((own - peak) * (SCALE * LOG2E))
            share = 1.0 / jnp.sum(before + own, -1, keepdims=True)
            shares = jnp.concatenate([before * share, own * share], axis=1).astype(BF16)
            sorted_out[pl.ds(c * SPAN, SPAN), :] = dot(shares, ordered[at, HD:]).astype(BF16)

    def leave(q):
        parts = []
        for b in range(2):
            j = q * 2 + b
            rows = sorted_out[pl.ds(j * TOK, TOK), :]
            parts.append(dot(leavehot[j], rows).reshape(NDEV // 2, 8, HD))
        pair = jnp.stack([halves(parts[0], parts[1]), halves(parts[1], parts[0])], axis=1)
        leaving[pl.ds(0, NDEV), q] = pair.reshape(NDEV, 8, HD).astype(BF16)

    def send_back(q):
        for o in every:
            tx, ty = at_offset(o)
            pltpu.make_async_remote_copy(
                leaving.at[tx * NSY + ty, q],
                returned.at[sy, sx, q],
                back_s.at[q],
                back_r.at[q],
                device_id=(tx, ty),
                device_id_type=MESH,
            ).start()
        returned[sy, sx, q] = leaving[me, q]

    def returns(q):
        back = whole(leaving.at[pl.ds(0, NDEV - 1), 0], back_s.at[q], back_r.at[q])
        back.wait_send()
        back.wait_recv()

    def merge(q, h):
        rows = returned[h, :, q].astype(F32).reshape(TOK // 4, HD).astype(BF16)
        return dot(mergehot[q, h], rows)

    with scope("wait_out0"):
        came(0)

    with scope("order0"):
        order(3, 1)
        order(3, 0)
        halo = pltpu.make_async_remote_copy(
            ordered.at[pl.ds(NPOS, SPAN)], ordered.at[pl.ds(0, SPAN)], halo_s, halo_r,
            device_id=(lax.rem(sx + 1, NSX), sy), device_id_type=MESH,
        )
        halo.start()
        order(2, 1)
        order(2, 0)

    with scope("attend0"):
        attend(17, 15)

    with scope("leave0"):
        leave(3)

    with scope("back0"):
        send_back(3)

    with scope("wait_out1"):
        came(1)

    with scope("order1"):
        order(1, 1)
        order(1, 0)

    with scope("attend1"):
        attend(9, 8)

    with scope("leave1"):
        leave(2)

    with scope("back1"):
        send_back(2)

    with scope("wait_out2"):
        came(2)

    with scope("order2"):
        order(0, 1)

    with scope("attend2"):
        attend(8, 1)

    with scope("leave2"):
        leave(1)

    with scope("back2"):
        send_back(1)

    with scope("order3"):
        order(0, 0)
        halo.wait_send()
        halo.wait_recv()
        units(ordered[pl.ds(0, SPAN), :HD].astype(F32), pl.ds(0, SPAN))

    with scope("attend3"):
        attend(0, 8)

    with scope("leave3"):
        leave(0)

    with scope("back3"):
        send_back(0)

    for q in (3, 2, 1):
        with scope(f"wait_back{q}"):
            returns(q)
        with scope(f"merge{q}"):
            for h in range(HEADS):
                partial[h] = merge(q, h) if q == 3 else partial[h] + merge(q, h)

    with scope("wait_back0"):
        returns(0)

    with scope("merge"):
        for h in range(HEADS):
            merged[:, h * HD : (h + 1) * HD] = (partial[h] + merge(0, h)).astype(BF16)


def per_device(tokens, norm_gain, w_qk, w_value, w_out, send_order, place):
    vmem = pl.BlockSpec(memory_space=pltpu.VMEM)
    hbm = pl.BlockSpec(memory_space=pltpu.HBM)
    dma = pltpu.SemaphoreType.DMA
    merged = pl.pallas_call(
        kernel,
        out_shape=jax.ShapeDtypeStruct((TOK, D), BF16),
        in_specs=[hbm] * 6,
        out_specs=vmem,
        scratch_shapes=[
            pltpu.VMEM((TOK, D), BF16),
            pltpu.VMEM((1, D), F32),
            pltpu.VMEM((HEADS, D, 2 * HD), BF16),
            pltpu.VMEM((HEADS, TOK), I32),
            pltpu.VMEM((HEADS, TOK), I32),
            pltpu.VMEM((TOK, D), BF16),
            pltpu.VMEM((HEADS + 1, NSX, 4, 8, 2 * HD), BF16),
            pltpu.VMEM((NDEV + 1, 4, 8, 2 * HD), BF16),
            pltpu.VMEM((NDEV + 1, 4, 8, HD), BF16),
            pltpu.VMEM((HEADS + 1, NSX, 4, 8, HD), BF16),
            pltpu.VMEM((2 * HEADS, 1, TOK), I32),
            pltpu.VMEM((2 * NSY, 1, TOK), I32),
            pltpu.VMEM((8, TOK), I32),
            pltpu.VMEM((8, TOK, 128), I32),
            pltpu.VMEM((8, TOK), I32),
            pltpu.VMEM((2, TOK, 2 * HD), BF16),
            pltpu.VMEM((4, 8, TOK // 4), I32),
            pltpu.VMEM((4, HEADS, TOK, TOK // 4), BF16),
            pltpu.VMEM((8, TOK, TOK), BF16),
            pltpu.VMEM((8, TOK, TOK), BF16),
            pltpu.VMEM((NPOS + SPAN, 2 * HD), BF16),
            pltpu.VMEM((NPOS + SPAN, HD), BF16),
            pltpu.VMEM((NPOS, HD), BF16),
            pltpu.VMEM((HEADS, TOK, HD), F32),
            dma((7,)),
            dma((HEADS, 2)),
            pltpu.SemaphoreType.REGULAR,
            dma, dma, dma((3,)), dma((3,)), dma, dma, dma((4,)), dma((4,)),
        ],
        compiler_params=pltpu.CompilerParams(
            collective_id=0, has_side_effects=True, vmem_limit_bytes=VMEM_LIMIT
        ),
    )(*[
        pltpu.with_memory_space_constraint(array, pltpu.HBM)
        for array in (tokens, norm_gain.reshape(1, D), w_qk, w_value, send_order, place)
    ])
    return jnp.dot(merged, w_out, preferred_element_type=F32).astype(BF16)


def solution(mesh):
    return jax.shard_map(
        per_device,
        mesh=mesh,
        in_specs=(P(("sx", "sy"), None), P(), P(), P(), P(), P(None, ("sx", "sy")), P(None, ("sx", "sy"))),
        out_specs=P(("sx", "sy"), None),
        check_vma=False,
    )
```
